8 devices in a mesh: dp: 1 (over z), cy: 2 (over y), cx: 2 (over x), core: 2 (over core).
Axes of the slice: x: 2, y: 2, z: 1, core: 2. Of those that a mesh axis runs over, the one named last changes fastest.
Arguments:
- x_in: bfloat16 [1, 1024, 2048], P('dp', ('cy', 'cx', 'core'))
- w_qkv: bfloat16 [2048, 40, 64], replicated
- w_out: bfloat16 [32, 64, 2048], replicated
Outputs:
- output: bfloat16 [1, 1024, 2048], P('dp', ('cy', 'cx', 'core'))
All inputs are finite; a program needn't handle non-finite values.
Results may differ from the reference program's by a relative error of at most 0.00798741.
Values are sent between devices in bfloat16 or wider.
A program may use at most 1 GiB of HBM per device.

```python
import math
import jax
import jax.numpy as jnp
from jax import lax

TOKENS_DEV = 128
GROUP_DEVICES = 8
HEADS = 32
KV_HEADS = 4
HEAD_DIM = 64

TOKENS = TOKENS_DEV * GROUP_DEVICES
WIDTH = HEADS * HEAD_DIM
GROUP_SIZE = HEADS // KV_HEADS
QUERY_GAIN = 2.0
OUT_GAIN = math.sqrt(TOKENS) * math.exp(-0.5 * QUERY_GAIN ** 2)


def setup_inputs(seed: int = 0, part: int = 0) -> dict:
    root_key = jax.random.key(seed)
    key_act = jax.random.fold_in(jax.random.fold_in(root_key, 1), part)
    key_qkv = jax.random.fold_in(root_key, 2)
    key_out = jax.random.fold_in(root_key, 3)
    act_rows = jax.random.normal(key_act, (1, TOKENS, WIDTH), jnp.float32)
    head_gain = jnp.concatenate([jnp.full((HEADS,), QUERY_GAIN, jnp.float32), jnp.ones((2 * KV_HEADS,), jnp.float32)])
    w_qkv = jax.random.normal(key_qkv, (WIDTH, HEADS + 2 * KV_HEADS, HEAD_DIM), jnp.float32) * (WIDTH ** -0.5) * head_gain[None, :, None]
    w_out = jax.random.normal(key_out, (HEADS, HEAD_DIM, WIDTH), jnp.float32) * (OUT_GAIN * WIDTH ** -0.5)
    return {"x_in": act_rows.astype(jnp.bfloat16), "w_qkv": w_qkv.astype(jnp.bfloat16), "w_out": w_out.astype(jnp.bfloat16)}


def reference(x_in, w_qkv, w_out):
    qkv_rows = jnp.dot(x_in[0], w_qkv.reshape(WIDTH, -1), preferred_element_type=jnp.float32)
    qkv_rows = qkv_rows.astype(jnp.bfloat16).reshape(TOKENS, HEADS + 2 * KV_HEADS, HEAD_DIM)
    queries = qkv_rows[:, :HEADS].reshape(GROUP_DEVICES, TOKENS_DEV, KV_HEADS, GROUP_SIZE, HEAD_DIM)
    queries = jnp.transpose(queries, (2, 0, 1, 3, 4))
    key_heads = jnp.transpose(qkv_rows[:, HEADS:HEADS + KV_HEADS], (1, 0, 2))
    value_heads = jnp.transpose(qkv_rows[:, HEADS + KV_HEADS:], (1, 0, 2))
    logit_scale = HEAD_DIM ** -0.5

    def head_attend(operands):
        q_head, k_head, v_head = operands
        k_wide = k_head.astype(jnp.float32)
        v_wide = v_head.astype(jnp.float32)

        def tile_attend(q_tile):
            scores = jnp.einsum("qgd,sd->gqs", q_tile.astype(jnp.float32), k_wide) * logit_scale
            weights = jax.nn.softmax(scores, axis=-1)
            return jnp.einsum("gqs,sd->qgd", weights, v_wide)

        return lax.map(tile_attend, q_head)

    attn_out = lax.map(head_attend, (queries, key_heads, value_heads))
    attn_out = jnp.transpose(attn_out, (1, 2, 0, 3, 4)).reshape(TOKENS, WIDTH).astype(jnp.bfloat16)
    y_rows = jnp.dot(attn_out, w_out.reshape(WIDTH, WIDTH), preferred_element_type=jnp.float32)
    return y_rows.astype(jnp.bfloat16)[None]
```

```python
import functools
import math

import jax
import jax.numpy as jnp
from jax import lax
from jax.experimental import pallas as pl
from jax.experimental.pallas import tpu as pltpu
from jax.sharding import PartitionSpec as P

MESH = pl.DeviceIdType.MESH
F32 = jnp.float32
BF16 = jnp.bfloat16

TOK = 128
WIDTH = 2048
HEADS = 32
KVH = 4
HD = 64
NKV = KVH * HD
QROWS = HEADS * HD
TILES = HEADS // 2
COLS = 2 * TOK
QCHUNKS = 4
OCHUNKS = 4
SCALE = (HD ** -0.5) * math.log2(math.e)


def kernel(x_hbm, wt_hbm, wo_hbm, y_hbm,
           x_v, xt_v, wkv_v, wq_v, wo_v, qp_v, k_v, vt_v, m_v, l_v, o_v, ob_v, y_v,
           x_sem, wkv_sem, wq_sem, wo_sem, y_sem, send_sem, recv_sem):
    cy = lax.axis_index("cy")
    cx = lax.axis_index("cx")
    co = lax.axis_index("core")
    partner = {"core": 1 - co}
    xnbr = {"cx": 1 - cx}
    ynbr = {"cy": 1 - cy}

    x_copy = pltpu.make_async_copy(x_hbm.at[0], x_v, x_sem)
    x_copy.start()
    wkv_copies = []
    for i in range(2):
        c = pltpu.make_async_copy(wt_hbm.at[pl.ds(QROWS + i * NKV, NKV)], wkv_v.at[i], wkv_sem.at[i])
        c.start()
        wkv_copies.append(c)
    qstep = QROWS // QCHUNKS
    wq_copies = []
    for i in range(QCHUNKS):
        c = pltpu.make_async_copy(wt_hbm.at[pl.ds(i * qstep, qstep)], wq_v.at[pl.ds(i * qstep, qstep)], wq_sem.at[i])
        c.start()
        wq_copies.append(c)
    ostep = WIDTH // OCHUNKS
    wo_copies = []
    for i in range(OCHUNKS):
        c = pltpu.make_async_copy(wo_hbm.at[pl.ds(i * ostep, ostep)], wo_v.at[pl.ds(i * ostep, ostep)], wo_sem.at[i])
        c.start()
        wo_copies.append(c)

    barrier = pltpu.get_barrier_semaphore()
    for peer in (partner, xnbr, ynbr):
        pl.semaphore_signal(barrier, inc=1, device_id=peer, device_id_type=MESH)

    qp_v[...] = jnp.zeros_like(qp_v)
    x_copy.wait()
    xt_v[...] = x_v[...].T

    wkv_copies[0].wait()
    k_own = lax.dot_general(x_v[...], wkv_v[0], (((1,), (1,)), ((), ())), preferred_element_type=F32)
    k_v[0, pl.ds(0, TOK), :] = k_own.astype(BF16)
    wkv_copies[1].wait()
    vt_own = jnp.dot(wkv_v[1], xt_v[...], preferred_element_type=F32)
    vt_v[0, 0, :, :] = vt_own.astype(BF16)

    pl.semaphore_wait(barrier, 3)

    def kref(phase, half):
        return k_v.at[phase, pl.ds(half * TOK, TOK)]

    def vref(phase, half):
        return vt_v.at[phase, half]

    def send(idx, src, dst, peer):
        c = pltpu.make_async_remote_copy(src_ref=src, dst_ref=dst, send_sem=send_sem.at[idx], recv_sem=recv_sem.at[idx],
                                         device_id=peer, device_id_type=MESH)
        return c

    kx = send(0, kref(0, 0), kref(1, 0), xnbr)
    vx = send(1, vref(0, 0), vref(1, 0), xnbr)
    vy = send(2, vref(0, 0), vref(2, 0), ynbr)
    ky = send(3, kref(0, 0), kref(2, 0), ynbr)
    kp = send(4, kref(0, 0), kref(0, 1), partner)
    vp = send(5, vref(0, 0), vref(0, 1), partner)
    for c in (kx, vy, vx, ky, kp, vp):
        c.start()
    kdiag = send(6, kref(1, 0), kref(3, 0), ynbr)
    vdiag = send(7, vref(2, 0), vref(3, 0), xnbr)
    kxp = send(8, kref(1, 0), kref(1, 1), partner)
    vxp = send(9, vref(1, 0), vref(1, 1), partner)
    kyp = send(10, kref(2, 0), kref(2, 1), partner)
    vyp = send(11, vref(2, 0), vref(2, 1), partner)
    kdp = send(12, kref(3, 0), kref(3, 1), partner)
    vdp = send(13, vref(3, 0), vref(3, 1), partner)

    for i in range(QCHUNKS):
        wq_copies[i].wait()
        qt = jnp.dot(wq_v[pl.ds(i * qstep, qstep), :], xt_v[...], preferred_element_type=F32).astype(BF16)
        heads_per = qstep // HD
        for h in range(heads_per):
            head = i * heads_per + h
            g = head // (HEADS // KVH)
            qp_v[head // 2, pl.ds(g * HD, HD), pl.ds((head % 2) * TOK, TOK)] = qt[h * HD:(h + 1) * HD]

    def attend(phase, first):
        keys = k_v.at[phase]

        def body(j, _):
            g = j // (TILES // KVH)
            s = jnp.dot(keys[...], qp_v[j], preferred_element_type=F32)
            smax = jnp.max(s, axis=0, keepdims=True) * SCALE
            if first:
                m_new = smax
            else:
                m_old = m_v[j]
                m_new = jnp.maximum(m_old, smax)
                alpha = jnp.exp2(m_old - m_new)
            p = jnp.exp2(s * SCALE - m_new)
            psum = jnp.sum(p, axis=0, keepdims=True)
            pb = p.astype(BF16)
            row = pl.multiple_of(g * HD, HD)
            pv = jnp.dot(vt_v[phase, 0, pl.ds(row, HD), :], pb[:TOK], preferred_element_type=F32)
            pv = pv + jnp.dot(vt_v[phase, 1, pl.ds(row, HD), :], pb[TOK:], preferred_element_type=F32)
            m_v[j] = m_new
            if first:
                l_v[j] = psum
                o_v[j] = pv
            else:
                l_v[j] = l_v[j] * alpha + psum
                o_v[j] = o_v[j] * alpha + pv
            return 0

        lax.fori_loop(0, TILES, body, 0, unroll=2)

    kp.wait_recv()
    vp.wait_recv()
    attend(0, True)

    kx.wait_recv()
    kdiag.start()
    kxp.start()
    vy.wait_recv()
    vdiag.start()
    vyp.start()
    vx.wait_recv()
    vxp.start()
    ky.wait_recv()
    kyp.start()
    kxp.wait_recv()
    vxp.wait_recv()
    attend(1, False)
    kdiag.wait_recv()
    kdp.start()
    vdiag.wait_recv()
    vdp.start()
    kyp.wait_recv()
    vyp.wait_recv()
    attend(2, False)
    kdp.wait_recv()
    vdp.wait_recv()
    attend(3, False)

    for j in range(TILES):
        inv = 1.0 / l_v[j]
        on = (o_v[j] * inv).astype(BF16)
        for e in range(2):
            head = 2 * j + e
            ob_v[pl.ds(head * HD, HD), :] = on[:, e * TOK:(e + 1) * TOK]
    o_rows = ob_v[...].T

    for c in wo_copies:
        c.wait()
    y_v[...] = jnp.dot(o_rows, wo_v[...], preferred_element_type=F32).astype(BF16)
    y_copy = pltpu.make_async_copy(y_v, y_hbm.at[0], y_sem)
    y_copy.start()
    y_copy.wait()
    for c in (kx, vx, vy, ky, kp, vp, kdiag, vdiag, kxp, vxp, kyp, vyp, kdp, vdp):
        c.wait_send()


def solution(mesh):
    seq_spec = P("dp", ("cy", "cx", "core"))

    def local_layer(x_loc, w_qkv, w_out):
        wt = jnp.transpose(w_qkv, (1, 2, 0)).reshape(QROWS + 2 * NKV, WIDTH)
        wo = w_out.reshape(QROWS, WIDTH)
        any_spec = pl.BlockSpec(memory_space=pl.ANY)
        return pl.pallas_call(
            kernel,
            out_shape=jax.ShapeDtypeStruct((1, TOK, WIDTH), BF16),
            in_specs=[any_spec] * 3,
            out_specs=any_spec,
            scratch_shapes=[
                pltpu.VMEM((TOK, WIDTH), BF16),
                pltpu.VMEM((WIDTH, TOK), BF16),
                pltpu.VMEM((2, NKV, WIDTH), BF16),
                pltpu.VMEM((QROWS, WIDTH), BF16),
                pltpu.VMEM((QROWS, WIDTH), BF16),
                pltpu.VMEM((TILES, NKV, COLS), BF16),
                pltpu.VMEM((4, 2 * TOK, NKV), BF16),
                pltpu.VMEM((4, 2, NKV, TOK), BF16),
                pltpu.VMEM((TILES, 1, COLS), F32),
                pltpu.VMEM((TILES, 1, COLS), F32),
                pltpu.VMEM((TILES, HD, COLS), F32),
                pltpu.VMEM((QROWS, TOK), BF16),
                pltpu.VMEM((TOK, WIDTH), BF16),
                pltpu.SemaphoreType.DMA,
                pltpu.SemaphoreType.DMA((2,)),
                pltpu.SemaphoreType.DMA((QCHUNKS,)),
                pltpu.SemaphoreType.DMA((OCHUNKS,)),
                pltpu.SemaphoreType.DMA,
                pltpu.SemaphoreType.DMA((14,)),
                pltpu.SemaphoreType.DMA((14,)),
            ],
            compiler_params=pltpu.CompilerParams(collective_id=0, has_side_effects=True, vmem_limit_bytes=60 * 1024 * 1024),
        )(x_loc, wt, wo)

    return jax.shard_map(local_layer, mesh=mesh, in_specs=(seq_spec, P(), P()), out_specs=seq_spec, check_vma=False)
```

```python
import functools
import math

import jax
import jax.numpy as jnp
from jax import lax
from jax.experimental import pallas as pl
from jax.experimental.pallas import tpu as pltpu
from jax.sharding import PartitionSpec as P

MESH = pl.DeviceIdType.MESH
F32 = jnp.float32
BF16 = jnp.bfloat16

TOK = 128
WIDTH = 2048
HEADS = 32
KVH = 4
HD = 64
NKV = KVH * HD
QROWS = HEADS * HD
TILES = HEADS // 2
COLS = 2 * TOK
QCHUNKS = 4
OCHUNKS = 4
NS = 3
NP = 3
SCALE = (HD ** -0.5) * math.log2(math.e)


def kernel(x_hbm, wt_hbm, wo_hbm, y_ref,
           x_v, xt_v, wkv_v, wq_v, wo_v, qp_v, k_v, vt_v, s_v, mp_v, p_v, m_v, al_v, l_v, o_v, ob_v,
           x_sem, wkv_sem, wq_sem, wo_sem, send_sem, recv_sem):
    cy = lax.axis_index("cy")
    cx = lax.axis_index("cx")
    co = lax.axis_index("core")
    partner = {"core": 1 - co}
    xnbr = {"cx": 1 - cx}
    ynbr = {"cy": 1 - cy}

    x_copy = pltpu.make_async_copy(x_hbm.at[0], x_v, x_sem)
    x_copy.start()
    wkv_copies = []
    for i in range(2):
        c = pltpu.make_async_copy(wt_hbm.at[pl.ds(QROWS + i * NKV, NKV)], wkv_v.at[i], wkv_sem.at[i])
        c.start()
        wkv_copies.append(c)

    barrier = pltpu.get_barrier_semaphore()
    for peer in (partner, xnbr, ynbr):
        pl.semaphore_signal(barrier, inc=1, device_id=peer, device_id_type=MESH)

    qstep = QROWS // QCHUNKS
    wq_copies = []
    for i in range(QCHUNKS):
        c = pltpu.make_async_copy(wt_hbm.at[pl.ds(i * qstep, qstep)], wq_v.at[pl.ds(i * qstep, qstep)], wq_sem.at[i])
        c.start()
        wq_copies.append(c)

    qp_v[...] = jnp.zeros_like(qp_v)
    x_copy.wait()
    xt_v[...] = x_v[...].T

    wkv_copies[0].wait()
    k_own = lax.dot_general(x_v[...], wkv_v[0], (((1,), (1,)), ((), ())), preferred_element_type=F32)
    k_v[pl.ds(0, TOK), :] = k_own.astype(BF16)
    wkv_copies[1].wait()
    v_own = lax.dot_general(x_v[...], wkv_v[1], (((1,), (1,)), ((), ())), preferred_element_type=F32)
    vt_v[:, pl.ds(0, TOK)] = v_own.astype(BF16).T

    pl.semaphore_wait(barrier, 3)

    def kref(slot):
        return k_v.at[pl.ds(slot * TOK, TOK)]

    def vref(slot):
        return vt_v.at[:, pl.ds(slot * TOK, TOK)]

    def send(idx, src, dst, peer):
        return pltpu.make_async_remote_copy(src_ref=src, dst_ref=dst, send_sem=send_sem.at[idx], recv_sem=recv_sem.at[idx],
                                            device_id=peer, device_id_type=MESH)

    kx = send(0, kref(0), kref(2), xnbr)
    vx = send(1, vref(0), vref(2), xnbr)
    vy = send(2, vref(0), vref(4), ynbr)
    ky = send(3, kref(0), kref(4), ynbr)
    kp = send(4, kref(0), kref(1), partner)
    vp = send(5, vref(0), vref(1), partner)
    for c in (kx, vy, vx, ky, kp, vp):
        c.start()
    kdiag = send(6, kref(2), kref(6), ynbr)
    vdiag = send(7, vref(4), vref(6), xnbr)
    kxp = send(8, kref(2), kref(3), partner)
    vxp = send(9, vref(2), vref(3), partner)
    kyp = send(10, kref(4), kref(5), partner)
    vyp = send(11, vref(4), vref(5), partner)
    kdp = send(12, kref(6), kref(7), partner)
    vdp = send(13, vref(6), vref(7), partner)

    ostep = WIDTH // OCHUNKS
    wo_copies = []
    for i in range(QCHUNKS):
        wq_copies[i].wait()
        if i == QCHUNKS - 1:
            for o in range(OCHUNKS):
                c = pltpu.make_async_copy(wo_hbm.at[pl.ds(o * ostep, ostep)], wo_v.at[pl.ds(o * ostep, ostep)], wo_sem.at[o])
                c.start()
                wo_copies.append(c)
        qt = jnp.dot(wq_v[pl.ds(i * qstep, qstep), :], xt_v[...], preferred_element_type=F32).astype(BF16)
        heads_per = qstep // HD
        for h in range(heads_per):
            head = i * heads_per + h
            g = head // (HEADS // KVH)
            qp_v[head // 2, pl.ds(g * HD, HD), pl.ds((head % 2) * TOK, TOK)] = qt[h * HD:(h + 1) * HD]

    def attend(slot, nk, first):
        k0 = slot * TOK

        def scores(j):
            s = jnp.dot(k_v[pl.ds(k0, nk), :], qp_v[j], preferred_element_type=F32)
            s_v[j % NS, pl.ds(0, nk), :] = s
            mp_v[j % NS] = jnp.max(s.reshape(nk // 8, 8, COLS), axis=0)

        def soft(j):
            m_new = jnp.max(mp_v[j % NS], axis=0, keepdims=True) * SCALE
            if not first:
                m_old = m_v[j]
                m_new = jnp.maximum(m_old, m_new)
                alpha = jnp.exp2(m_old - m_new)
                al_v[j] = alpha
            m_v[j] = m_new
            p = jnp.exp2(s_v[j % NS, pl.ds(0, nk), :] * SCALE - m_new)
            psum = jnp.sum(p.reshape(nk // 8, 8, COLS), axis=0)
            l_v[j] = psum if first else l_v[j] * alpha + psum
            p_v[j % NP, pl.ds(0, nk), :] = p.astype(BF16)

        def mix(j):
            g = j // (TILES // KVH)
            pv = jnp.dot(vt_v[pl.ds(g * HD, HD), pl.ds(k0, nk)], p_v[j % NP, pl.ds(0, nk), :], preferred_element_type=F32)
            o_v[j] = pv if first else o_v[j] * al_v[j] + pv

        for t in range(TILES + 2):
            if t < TILES:
                scores(t)
            if 0 <= t - 1 < TILES:
                soft(t - 1)
            if 0 <= t - 2 < TILES:
                mix(t - 2)

    kp.wait_recv()
    vp.wait_recv()
    attend(0, 2 * TOK, True)

    kx.wait_recv()
    kdiag.start()
    kxp.start()
    vy.wait_recv()
    vdiag.start()
    vyp.start()
    vx.wait_recv()
    vxp.start()
    ky.wait_recv()
    kyp.start()
    kxp.wait_recv()
    vxp.wait_recv()
    kyp.wait_recv()
    vyp.wait_recv()
    attend(2, 4 * TOK, False)
    kdiag.wait_recv()
    kdp.start()
    vdiag.wait_recv()
    vdp.start()
    kdp.wait_recv()
    vdp.wait_recv()
    attend(6, 2 * TOK, False)

    for j in range(TILES):
        inv = 1.0 / jnp.sum(l_v[j], axis=0, keepdims=True)
        on = (o_v[j] * inv).astype(BF16)
        for e in range(2):
            head = 2 * j + e
            ob_v[pl.ds(head * HD, HD), :] = on[:, e * TOK:(e + 1) * TOK]
    o_rows = ob_v[...].T

    for c in wo_copies:
        c.wait()
    y_ref[0] = jnp.dot(o_rows, wo_v[...], preferred_element_type=F32).astype(BF16)
    for c in (kx, vx, vy, ky, kp, vp, kdiag, vdiag, kxp, vxp, kyp, vyp, kdp, vdp):
        c.wait_send()


def solution(mesh):
    seq_spec = P("dp", ("cy", "cx", "core"))

    def local_layer(x_loc, w_qkv, w_out):
        wt = jnp.transpose(w_qkv, (1, 2, 0)).reshape(QROWS + 2 * NKV, WIDTH)
        wo = w_out.reshape(QROWS, WIDTH)
        any_spec = pl.BlockSpec(memory_space=pl.ANY)
        return pl.pallas_call(
            kernel,
            out_shape=jax.ShapeDtypeStruct((1, TOK, WIDTH), BF16),
            in_specs=[any_spec] * 3,
            out_specs=pl.BlockSpec(memory_space=pltpu.VMEM),
            scratch_shapes=[
                pltpu.VMEM((TOK, WIDTH), BF16),
                pltpu.VMEM((WIDTH, TOK), BF16),
                pltpu.VMEM((2, NKV, WIDTH), BF16),
                pltpu.VMEM((QROWS, WIDTH), BF16),
                pltpu.VMEM((QROWS, WIDTH), BF16),
                pltpu.VMEM((TILES, NKV, COLS), BF16),
                pltpu.VMEM((8 * TOK, NKV), BF16),
                pltpu.VMEM((NKV, 8 * TOK), BF16),
                pltpu.VMEM((NS, 4 * TOK, COLS), F32),
                pltpu.VMEM((NS, 8, COLS), F32),
                pltpu.VMEM((NP, 4 * TOK, COLS), BF16),
                pltpu.VMEM((TILES, 1, COLS), F32),
                pltpu.VMEM((TILES, 1, COLS), F32),
                pltpu.VMEM((TILES, 8, COLS), F32),
                pltpu.VMEM((TILES, HD, COLS), F32),
                pltpu.VMEM((QROWS, TOK), BF16),
                pltpu.SemaphoreType.DMA,
                pltpu.SemaphoreType.DMA((2,)),
                pltpu.SemaphoreType.DMA((QCHUNKS,)),
                pltpu.SemaphoreType.DMA((OCHUNKS,)),
                pltpu.SemaphoreType.DMA((14,)),
                pltpu.SemaphoreType.DMA((14,)),
            ],
            compiler_params=pltpu.CompilerParams(collective_id=0, has_side_effects=True, vmem_limit_bytes=60 * 1024 * 1024),
        )(x_loc, wt, wo)

    return jax.shard_map(local_layer, mesh=mesh, in_specs=(seq_spec, P(), P()), out_specs=seq_spec, check_vma=False)
```
